1024 devices in a mesh: dp: 16 (over y_lo, x, core), mp: 64 (over z, y_hi).
Axes of the slice: x: 4, y: 4 (y_hi: 2, y_lo: 2; y = y_hi * 2 + y_lo), z: 32, core: 2. Of those that a mesh axis runs over, the one named last changes fastest.
Arguments:
- cotangent: bfloat16 [2048, 4608], P(('dp', 'mp')), may hold values from -50 to 50
- mlp_out: bfloat16 [2048, 4608], P(('dp', 'mp')), may hold values from -500 to 500
- post_gain: float32 [4608], replicated, may hold values from 0.5 to 1.5
- down_weight: bfloat16 [36864, 4608], P('mp', 'dp'), may hold values from -0.09375 to 0.09375
- gate_pre: bfloat16 [2048, 36864], P('dp', 'mp'), may hold values from -6 to 6
- up_pre: bfloat16 [2048, 36864], P('dp', 'mp'), may hold values from -6 to 6
Outputs:
- gate_grad: float32 [2048, 36864], P('dp', 'mp')
- up_grad: float32 [2048, 36864], P('dp', 'mp')
- gain_grad: float32 [4608], replicated
The draws below stay inside these ranges and needn't reach their ends.
All inputs are finite; a program needn't handle non-finite values.
Results may differ from the reference program's by a relative error of at most 0.0005.
Values may be sent and summed in bfloat16 or wider, within the bound.
No kernel may reach another device: no remote copies, remote signals or barrier semaphores. Data moves between devices by JAX's collectives and lax.ppermute only.
A program may use at most 32 MiB of HBM per device.

```python
import jax
import jax.numpy as jnp
from jax import lax

D = 4608
FF = 36864
TOKENS = 2048


def draw_cotangent(key, part):
    noise_key, jitter_key = jax.random.split(jax.random.fold_in(key, 17))
    row_pos = jnp.arange(TOKENS, dtype=jnp.float32)[:, None] / TOKENS
    jitter = jax.random.uniform(jitter_key, (TOKENS, 1), jnp.float32)
    values = jnp.clip(jax.random.normal(noise_key, (TOKENS, D), jnp.float32), -5.0, 5.0)
    row_exp = 0.5 * row_pos + 0.5 * jitter
    return (values * 10.0 ** row_exp).astype(jnp.bfloat16)


def draw_mlp_out(key, part):
    noise_key, row_key, col_key = jax.random.split(jax.random.fold_in(key, 29), 3)
    row_exp = jax.random.uniform(row_key, (TOKENS, 1), jnp.float32)
    col_exp = jax.random.uniform(col_key, (1, D), jnp.float32)
    values = jnp.clip(jax.random.normal(noise_key, (TOKENS, D), jnp.float32), -5.0, 5.0)
    return (values * 10.0 ** row_exp * 10.0 ** col_exp).astype(jnp.bfloat16)


def steps_of(own_key, shape, cuts, smallest, top_value):
    loudness = 1.0
    for dim, parts in cuts:
        heights = jax.random.uniform(jax.random.fold_in(jax.random.fold_in(own_key, 6), dim), (parts,), jnp.float32, smallest / len(cuts), top_value / len(cuts))
        loudness = loudness * jnp.repeat(jnp.exp(heights), shape[dim] // parts).reshape((-1,) + (1,) * (len(shape) - 1 - dim))
    return loudness


def bell_draw(rng, shape, deviation, most, cuts=(), kind=jnp.bfloat16):
    values = jax.random.normal(rng, shape, jnp.float32) * deviation
    if len(cuts) > 0:
        values = steps_of(rng, shape, cuts, -0.22, 0.18) * values
    return jnp.clip(values, min=-most, max=most).astype(kind)


def setup_inputs(seed: int = 0) -> dict:
    arg_keys = jax.random.split(jax.random.key(seed), 7)
    cotangent = draw_cotangent(jax.random.fold_in(arg_keys[6], 71), 0)
    mlp_out = draw_mlp_out(jax.random.fold_in(arg_keys[6], 71), 0)
    post_gain = jnp.clip(1.0 + 0.1 * jax.random.normal(arg_keys[2], (D,), jnp.float32), 0.5, 1.5)
    down_weight = bell_draw(arg_keys[3], (FF, D), D ** -0.5, 0.09375, ((0, 64), (1, 16)))
    gate_pre = bell_draw(arg_keys[4], (TOKENS, FF), 1.0, 6.0, ((0, 16), (1, 64)))
    up_pre = bell_draw(arg_keys[5], (TOKENS, FF), 1.0, 6.0, ((0, 16), (1, 64)))
    return {"cotangent": cotangent, "mlp_out": mlp_out, "post_gain": post_gain, "down_weight": down_weight, "gate_pre": gate_pre, "up_pre": up_pre}


epsilon = 1e-06

def gelu_tanh(values):
    return jax.nn.gelu(values, approximate=True)

def reference(cotangent, mlp_out, post_gain, down_weight, gate_pre, up_pre):
    forward = mlp_out.astype(jnp.float32)
    upstream = cotangent.astype(jnp.float32)
    root_mean = jnp.sqrt(lax.optimization_barrier(jnp.mean(forward * forward, axis=1, keepdims=True)) + epsilon)
    normed = forward / root_mean
    gain_grad = lax.optimization_barrier(jnp.sum(upstream * normed, axis=0))
    scaled = upstream * post_gain[None, :]
    project_sum = lax.optimization_barrier(jnp.sum(scaled * forward, axis=1, keepdims=True))
    out_grad = scaled / root_mean - forward * project_sum / (D * root_mean ** 3)
    hidden_grad = jnp.dot(out_grad, down_weight.astype(jnp.float32).T, precision=lax.Precision.HIGHEST)
    gate_val = gate_pre.astype(jnp.float32)
    up_val = up_pre.astype(jnp.float32)
    act_val, pull_back = jax.vjp(gelu_tanh, gate_val)
    gate_grad = pull_back(hidden_grad * up_val)[0]
    up_grad = hidden_grad * act_val
    return (gate_grad, up_grad, gain_grad)
```

```python
import functools

import jax
import jax.numpy as jnp
from jax import lax
from jax.experimental import pallas as pl
from jax.experimental.pallas import tpu as pltpu
from jax.sharding import Mesh
from jax.sharding import PartitionSpec as P

D = 4608
DP = ("yl", "x", "c")
MP = ("zs", "zl", "yh")
ALL = DP + MP
PLANE = ("yl", "x", "c", "yh")
epsilon = 1e-06

LANES = 128
KT = D // LANES
ROWS = 80
ZS, ZL = 8, 4
HALF = ZS * ZL * ROWS


def pre_kernel(c_ref, y_ref, g_ref, q_ref, gp_ref):
    y = y_ref[...].astype(jnp.float32)
    c = c_ref[...].astype(jnp.float32)
    rm = jnp.sqrt(jnp.sum(y * y, axis=1, keepdims=True) / D + epsilon)
    gp = jnp.sum(c * (y / rm), axis=0, keepdims=True)
    scaled = c * g_ref[...]
    ps = jnp.sum(scaled * y, axis=1, keepdims=True)
    og = scaled / rm - y * (ps / (D * (rm * rm * rm)))
    top = jnp.max(jnp.abs(og), axis=1, keepdims=True)
    e = jnp.clip(jnp.ceil(jnp.log2(jnp.maximum(top, 1e-37))), -100.0, 100.0)
    q = og * jnp.exp2(-e)
    for k in range(KT):
        q_ref[2 * k : 2 * k + 2, :] = q[:, LANES * k : LANES * (k + 1)]
        gp_ref[k : k + 1, :] = gp[:, LANES * k : LANES * (k + 1)]
    q_ref[2 * KT : 2 * KT + 2, :] = jnp.broadcast_to(e, (2, LANES))
    q_ref[2 * KT + 2 :, :] = jnp.zeros((ROWS - 2 * KT - 2, LANES), jnp.float32)
    gp_ref[KT:, :] = jnp.zeros((64 - KT, LANES), jnp.float32)


KSTEP = 4
NSTEP = KT // KSTEP


def main_kernel(yh_ref, own_ref, rec_ref, w_ref, gate_ref, up_ref, gg_ref, ug_ref, acc_ref, nat_ref):
    step = pl.program_id(0)
    members = ZS * ZL

    @pl.when(step == 0)
    def _():
        acc_ref[...] = jnp.zeros_like(acc_ref)

    scales = [
        jnp.exp2(ref[pl.ds(2 * KT + r, members, stride=ROWS), :])
        for ref in (own_ref, rec_ref)
        for r in range(2)
    ]
    his, los = [], []
    for kk in range(KSTEP):
        hi_col, lo_col = [], []
        for h, ref in enumerate((own_ref, rec_ref)):
            for r in range(2):
                start = 2 * (step * KSTEP + kk) + r
                x = ref[pl.ds(start, members, stride=ROWS), :] * scales[2 * h + r]
                hi = x.astype(jnp.bfloat16)
                hi_col.append(hi)
                lo_col.append((x - hi.astype(jnp.float32)).astype(jnp.bfloat16))
        his.append(jnp.concatenate(hi_col, axis=0))
        los.append(jnp.concatenate(lo_col, axis=0))
    x_all = jnp.concatenate(
        [jnp.concatenate(his, axis=1), jnp.concatenate(los, axis=1)], axis=0
    )
    acc_ref[...] += jnp.dot(x_all, w_ref[...], preferred_element_type=jnp.float32)

    @pl.when(step == NSTEP - 1)
    def _():
        hid = acc_ref[: 4 * members, :] + acc_ref[4 * members :, :]
        n = hid.shape[1]

        def place(first):
            for b in range(4):
                h, r = divmod(b, 2)
                yh = first if h == 0 else 1 - first
                for zl in range(ZL):
                    row = b * members + zl * ZS
                    for j in range(0, n, LANES):
                        part = hid[row : row + ZS, j : min(j + LANES, n)]
                        if part.shape[1] < LANES:
                            part = jnp.concatenate([part, jnp.zeros((ZS, LANES - part.shape[1]), jnp.float32)], axis=1)
                        nat_ref[j // LANES, pl.ds(zl * 4 + yh * 2 + r, ZS, stride=16), :] = part

        @pl.when(yh_ref[0] == 0)
        def _():
            place(0)

        @pl.when(yh_ref[0] != 0)
        def _():
            place(1)

        for j in range(0, n, LANES):
            w = min(LANES, n - j)
            hidden = nat_ref[j // LANES].T[:w]
            g = gate_ref[j : j + w, :].astype(jnp.float32)
            u = up_ref[j : j + w, :].astype(jnp.float32)
            k0 = 0.7978845608028654
            g2 = g * g
            t = jnp.tanh(k0 * (g + 0.044715 * (g2 * g)))
            half = 0.5 * (1.0 + t)
            slope = half + (0.5 * k0) * g * (1.0 - t * t) * (1.0 + (3 * 0.044715) * g2)
            gg_ref[j : j + w, :] = hidden * u * slope
            ug_ref[j : j + w, :] = hidden * (g * half)


def run_main(yh, own, rec, weight, gate, up, interpret=False):
    n, rows = gate.shape
    whole = lambda s: pl.BlockSpec(s, lambda i: (0, 0))
    return pl.pallas_call(
        main_kernel,
        grid=(NSTEP,),
        in_specs=[
            pl.BlockSpec(memory_space=pltpu.SMEM),
            whole((HALF, LANES)),
            whole((HALF, LANES)),
            pl.BlockSpec((KSTEP * LANES, n), lambda i: (i, 0)),
            whole((n, rows)),
            whole((n, rows)),
        ],
        out_specs=[whole((n, rows)), whole((n, rows))],
        out_shape=(
            jax.ShapeDtypeStruct((n, rows), jnp.float32),
            jax.ShapeDtypeStruct((n, rows), jnp.float32),
        ),
        scratch_shapes=[
            pltpu.VMEM((8 * ZS * ZL, n), jnp.float32),
            pltpu.VMEM(((n + LANES - 1) // LANES, rows, LANES), jnp.float32),
        ],
        name="main",
        interpret=interpret,
    )(yh, own, rec, weight, gate, up)


def spread(v, axes):
    n = lax.axis_size(axes)
    return lax.all_to_all(jnp.broadcast_to(v[None], (n,) + v.shape), axes, 0, 0, tiled=True)


def local(cotangent, mlp_out, post_gain, down_weight, gate_pre, up_pre):
    weight = lax.all_gather(down_weight.T, DP, axis=0, tiled=True)
    q, gain_part = pl.pallas_call(
        pre_kernel,
        out_shape=(
            jax.ShapeDtypeStruct((ROWS, LANES), jnp.float32),
            jax.ShapeDtypeStruct((64, LANES), jnp.float32),
        ),
        name="pre",
    )(cotangent, mlp_out, post_gain.reshape(1, D))
    gain_rows = lax.all_to_all(gain_part.reshape(32, 2, LANES), PLANE, 0, 0, tiled=True)
    gain_rows = jnp.sum(gain_rows, axis=0)
    top = jnp.max(jnp.abs(gain_rows))
    ge = jnp.clip(jnp.ceil(jnp.log2(jnp.maximum(top, 1e-37))), -100.0, 100.0)
    gx = gain_rows * jnp.exp2(-ge)
    ghi = lax.reduce_precision(gx, 5, 10)
    glo = (gx - ghi) * 2048.0
    message = jnp.concatenate(
        [q[: 2 * KT + 2], ghi, glo, jnp.full((2, LANES), ge)], axis=0
    ).astype(jnp.float16)
    b1 = spread(message, ("zs",)).reshape(ZS * ROWS, LANES)
    b2 = spread(b1, ("zl",)).reshape(HALF, LANES)
    other = lax.ppermute(b2, "yh", [(0, 1), (1, 0)])
    extra = b2.reshape(ZS * ZL, ROWS, LANES)[:, 2 * KT + 2 :].astype(jnp.float32)
    gain_sum = jnp.sum(
        (extra[:, 0:2] + extra[:, 2:4] * (1.0 / 2048.0)) * jnp.exp2(extra[:, 4:6]), axis=0
    )
    gain_grad = spread(gain_sum, PLANE).reshape(64 * LANES)[:D]
    gate_grad, up_grad = run_main(
        lax.axis_index("yh").reshape(1),
        b2.astype(jnp.float32),
        other.astype(jnp.float32),
        weight,
        gate_pre.T,
        up_pre.T,
    )
    return (gate_grad.T, up_grad.T, gain_grad)


def solution(mesh):
    finer = Mesh(mesh.devices.reshape(2, 4, 2, ZS, ZL, 2), ALL)
    in_specs = (P(ALL, None), P(ALL, None), P(), P(MP, DP), P(DP, MP), P(DP, MP))
    out_specs = (P(DP, MP), P(DP, MP), P())
    return jax.shard_map(local, mesh=finer, in_specs=in_specs, out_specs=out_specs, check_vma=False)
```

```python
import jax
import jax.numpy as jnp
from jax import lax
from jax.experimental import pallas as pl
from jax.experimental.pallas import tpu as pltpu
from jax.sharding import Mesh
from jax.sharding import PartitionSpec as P


D = 4608
DP = ("yl", "x", "c")
MP = ("z", "yh")
ALL = DP + MP
PLANE = ("yl", "x", "c", "yh")
epsilon = 1e-06

LANES = 128
KT = D // LANES
ROWS = 80
GROWS = 80
Z = 32
LOW = 256.0


def pre_kernel(c_ref, y_ref, g_ref, m_ref):
    y = y_ref[...].astype(jnp.float32)
    c = c_ref[...].astype(jnp.float32)
    gain = jnp.broadcast_to(g_ref[...].reshape(1, D), (1, D))
    rm = jnp.sqrt(jnp.sum(y * y, axis=1, keepdims=True) / D + epsilon)
    gp = jnp.sum(c * (y / rm), axis=0, keepdims=True)
    scaled = c * gain
    ps = jnp.sum(scaled * y, axis=1, keepdims=True)
    og = scaled / rm - y * (ps / (D * (rm * rm * rm)))
    top = jnp.max(jnp.abs(og), axis=1, keepdims=True)
    e = jnp.clip(jnp.ceil(jnp.log2(jnp.maximum(top, 1e-37))), -100.0, 100.0)
    q = og * jnp.exp2(-e)
    gtop = jnp.max(jnp.abs(gp), axis=1, keepdims=True)
    ge = jnp.clip(jnp.ceil(jnp.log2(jnp.maximum(gtop, 1e-37))), -100.0, 100.0)
    gx = gp * jnp.exp2(-ge)
    hi = gx.astype(jnp.bfloat16).astype(jnp.float32)
    lo = (gx - hi) * LOW
    for k in range(KT):
        m_ref[2 * k : 2 * k + 2, :] = q[:, LANES * k : LANES * (k + 1)]
        m_ref[ROWS + k : ROWS + k + 1, :] = hi[:, LANES * k : LANES * (k + 1)]
        m_ref[ROWS + KT + k : ROWS + KT + k + 1, :] = lo[:, LANES * k : LANES * (k + 1)]
    m_ref[2 * KT : 2 * KT + 2, :] = jnp.broadcast_to(e, (2, LANES))
    m_ref[2 * KT + 2 : ROWS, :] = jnp.zeros((ROWS - 2 * KT - 2, LANES), jnp.float32)
    m_ref[ROWS + 2 * KT : ROWS + 2 * KT + 1, :] = jnp.broadcast_to(ge, (1, LANES))
    m_ref[ROWS + 2 * KT + 1 :, :] = jnp.zeros((GROWS - 2 * KT - 1, LANES), jnp.float32)


KSTEP = 12
NSTEP = KT // KSTEP


def products(src_ref, w_ref, acc_ref):
    step = pl.program_id(0)

    @pl.when(step == 0)
    def _():
        acc_ref[...] = jnp.zeros_like(acc_ref)

    scales = [jnp.exp2(src_ref[pl.ds(2 * KT + r, Z, stride=ROWS), :]) for r in range(2)]
    his, los = [], []
    for kk in range(KSTEP):
        x = jnp.concatenate(
            [src_ref[pl.ds(2 * (step * KSTEP + kk) + r, Z, stride=ROWS), :] * scales[r] for r in range(2)], axis=0
        )
        hi = x.astype(jnp.bfloat16)
        his.append(hi)
        los.append((x - hi.astype(jnp.float32)).astype(jnp.bfloat16))
    x_all = jnp.concatenate([jnp.concatenate(his, axis=1), jnp.concatenate(los, axis=1)], axis=0)
    acc_ref[...] += jnp.dot(x_all, w_ref[...], preferred_element_type=jnp.float32)


def own_kernel(own_ref, w_ref, out_ref, acc_ref):
    products(own_ref, w_ref, acc_ref)

    @pl.when(pl.program_id(0) == NSTEP - 1)
    def _():
        out_ref[...] = acc_ref[: 2 * Z, :] + acc_ref[2 * Z :, :]


def last_kernel(yh_ref, rec_ref, w_ref, own_ref, gate_ref, up_ref, gg_ref, ug_ref, acc_ref, nat_ref):
    products(rec_ref, w_ref, acc_ref)

    @pl.when(pl.program_id(0) == NSTEP - 1)
    def _():
        n = acc_ref.shape[1]
        yh = yh_ref[0]
        halves = (own_ref[...], acc_ref[: 2 * Z, :] + acc_ref[2 * Z :, :])
        for j in range(0, n, LANES):
            w = min(LANES, n - j)
            for h in range(2):
                at = yh if h == 0 else 1 - yh
                for r in range(2):
                    part = halves[h][r * Z : (r + 1) * Z, j : j + w]
                    if w < LANES:
                        part = jnp.concatenate([part, jnp.zeros((Z, LANES - w), jnp.float32)], axis=1)
                    nat_ref[j // LANES, pl.ds(at * 2 + r, Z, stride=4), :] = part
            hidden = nat_ref[j // LANES].T[:w]
            g = gate_ref[j : j + w, :].astype(jnp.float32)
            u = up_ref[j : j + w, :].astype(jnp.float32)
            k0 = 0.7978845608028654
            g2 = g * g
            t = jnp.tanh(k0 * (g + 0.044715 * (g2 * g)))
            half = 0.5 * (1.0 + t)
            slope = half + (0.5 * k0) * g * (1.0 - t * t) * (1.0 + (3 * 0.044715) * g2)
            gg_ref[j : j + w, :] = hidden * u * slope
            ug_ref[j : j + w, :] = hidden * (g * half)


def whole(*shape):
    return pl.BlockSpec(shape, lambda i: (0,) * len(shape))


def run_own(own, weight, interpret=False):
    n = weight.shape[1]
    return pl.pallas_call(
        own_kernel,
        grid=(NSTEP,),
        in_specs=[whole(Z * ROWS, LANES), pl.BlockSpec((KSTEP * LANES, n), lambda i: (i, 0))],
        out_specs=whole(2 * Z, n),
        out_shape=jax.ShapeDtypeStruct((2 * Z, n), jnp.float32),
        scratch_shapes=[pltpu.VMEM((4 * Z, n), jnp.float32)],
        cost_estimate=pl.CostEstimate(flops=4 * 2 * Z * n * D, transcendentals=0, bytes_accessed=2 * n * D),
        name="own",
        interpret=interpret,
    )(own, weight)


def run_last(yh, rec, weight, own, gate, up, interpret=False):
    n, rows = gate.shape
    shape = jax.ShapeDtypeStruct((n, rows), jnp.float32)
    return pl.pallas_call(
        last_kernel,
        grid=(NSTEP,),
        in_specs=[
            pl.BlockSpec(memory_space=pltpu.SMEM),
            whole(Z * ROWS, LANES),
            pl.BlockSpec((KSTEP * LANES, n), lambda i: (i, 0)),
            whole(2 * Z, n),
            whole(n, rows),
            whole(n, rows),
        ],
        out_specs=[whole(n, rows), whole(n, rows)],
        out_shape=(shape, shape),
        scratch_shapes=[
            pltpu.VMEM((4 * Z, n), jnp.float32),
            pltpu.VMEM(((n + LANES - 1) // LANES, rows, LANES), jnp.float32),
        ],
        name="last",
        interpret=interpret,
    )(yh, rec, weight, own, gate, up)


def spread(v, axes):
    n = lax.axis_size(axes)
    return lax.all_to_all(jnp.broadcast_to(v[None], (n,) + v.shape), axes, 0, 0, tiled=True)


def steps(cotangent, mlp_out, post_gain, down_weight, gate_pre, up_pre):
    weight = lax.all_gather(down_weight.T, DP, axis=0, tiled=True)
    message = pl.pallas_call(
        pre_kernel,
        out_shape=jax.ShapeDtypeStruct((ROWS + GROWS, LANES), jnp.float32),
        name="pre",
    )(cotangent, mlp_out, post_gain)
    got = lax.all_gather(message.astype(jnp.float16), "z", axis=0)
    own = got[:, :ROWS].reshape(Z * ROWS, LANES)
    other = lax.ppermute(own, "yh", [(0, 1), (1, 0)])
    terms = got[:, ROWS:].astype(jnp.float32)
    gain = jnp.sum(
        (terms[:, :KT] + terms[:, KT : 2 * KT] * (1.0 / LOW)) * jnp.exp2(terms[:, 2 * KT : 2 * KT + 1]), axis=0
    )
    parts = spread(gain, PLANE)
    gain_grad = jnp.sum(parts, axis=0).reshape(D)
    hidden = run_own(own.astype(jnp.float32), weight)
    gate_grad, up_grad = run_last(
        lax.axis_index("yh").reshape(1), other.astype(jnp.float32), weight, hidden, gate_pre.T, up_pre.T
    )
    return (gate_grad.T, up_grad.T, gain_grad)


def solution(mesh):
    finer = Mesh(mesh.devices.reshape(2, 4, 2, Z, 2), ALL)
    in_specs = (P(ALL, None), P(ALL, None), P(), P(MP, DP), P(DP, MP), P(DP, MP))
    out_specs = (P(DP, MP), P(DP, MP), P())
    return jax.shard_map(steps, mesh=finer, in_specs=in_specs, out_specs=out_specs, check_vma=False)
```

```python
import jax
import jax.numpy as jnp
from jax import lax
from jax.experimental import pallas as pl
from jax.experimental.pallas import tpu as pltpu
from jax.sharding import Mesh
from jax.sharding import PartitionSpec as P


D = 4608
DP = ("yl", "x", "c")
MP = ("z", "yh")
ALL = DP + MP
PLANE = ("yl", "x", "c", "yh")
epsilon = 1e-06

LANES = 128
KT = D // LANES
ROWS = 80
GROWS = 80
Z = 32
LOW = 256.0
VMEM = 20 << 20
STAGE_VMEM = 46 << 20


def pre_kernel(c_hbm, y_hbm, g_hbm, m_ref, c_ref, y_ref, g_ref, sems):
    pairs = ((c_hbm, c_ref), (y_hbm, y_ref), (g_hbm, g_ref))
    copies = [pltpu.make_async_copy(src, dst, sems.at[i]) for i, (src, dst) in enumerate(pairs)]
    for copy in copies:
        copy.start()
    for copy in copies:
        copy.wait()
    y = y_ref[...].astype(jnp.float32)
    c = c_ref[...].astype(jnp.float32)
    gain = jnp.broadcast_to(g_ref[...].reshape(1, D), (1, D))
    rm = jnp.sqrt(jnp.sum(y * y, axis=1, keepdims=True) / D + epsilon)
    gp = jnp.sum(c * (y / rm), axis=0, keepdims=True)
    scaled = c * gain
    ps = jnp.sum(scaled * y, axis=1, keepdims=True)
    og = scaled / rm - y * (ps / (D * (rm * rm * rm)))
    top = jnp.max(jnp.abs(og), axis=1, keepdims=True)
    e = jnp.clip(jnp.ceil(jnp.log2(jnp.maximum(top, 1e-37))), -100.0, 100.0)
    q = og * jnp.exp2(-e)
    gtop = jnp.max(jnp.abs(gp), axis=1, keepdims=True)
    ge = jnp.clip(jnp.ceil(jnp.log2(jnp.maximum(gtop, 1e-37))), -100.0, 100.0)
    gx = gp * jnp.exp2(-ge)
    hi = gx.astype(jnp.bfloat16).astype(jnp.float32)
    lo = (gx - hi) * LOW
    for k in range(KT):
        m_ref[2 * k : 2 * k + 2, :] = q[:, LANES * k : LANES * (k + 1)]
        m_ref[ROWS + k : ROWS + k + 1, :] = hi[:, LANES * k : LANES * (k + 1)]
        m_ref[ROWS + KT + k : ROWS + KT + k + 1, :] = lo[:, LANES * k : LANES * (k + 1)]
    m_ref[2 * KT : 2 * KT + 2, :] = jnp.broadcast_to(e, (2, LANES))
    m_ref[2 * KT + 2 : ROWS, :] = jnp.zeros((ROWS - 2 * KT - 2, LANES), jnp.float32)
    m_ref[ROWS + 2 * KT : ROWS + 2 * KT + 1, :] = jnp.broadcast_to(ge, (1, LANES))
    m_ref[ROWS + 2 * KT + 1 :, :] = jnp.zeros((GROWS - 2 * KT - 1, LANES), jnp.float32)


KSTEP = 12
NSTEP = KT // KSTEP


def parts(src_ref, step):
    scales = [jnp.exp2(src_ref[pl.ds(2 * KT + r, Z, stride=ROWS), :]) for r in range(2)]
    his, los = [], []
    for kk in range(KSTEP):
        x = jnp.concatenate(
            [src_ref[pl.ds(2 * (step * KSTEP + kk) + r, Z, stride=ROWS), :] * scales[r] for r in range(2)], axis=0
        )
        hi = x.astype(jnp.bfloat16)
        his.append(hi)
        los.append((x - hi.astype(jnp.float32)).astype(jnp.bfloat16))
    return jnp.concatenate([jnp.concatenate(his, axis=1), jnp.concatenate(los, axis=1)], axis=0)


def factor_kernel(w_hbm, gate_ref, up_ref, w_out, ga_ref, ua_ref, sem):
    copy = pltpu.make_async_copy(w_hbm, w_out, sem)
    copy.start()
    g = gate_ref[...].astype(jnp.float32)
    u = up_ref[...].astype(jnp.float32)
    k0 = 0.7978845608028654
    g2 = g * g
    t = jnp.tanh(k0 * (g + 0.044715 * (g2 * g)))
    half = 0.5 * (1.0 + t)
    ga_ref[...] = u * (half + (0.5 * k0) * g * (1.0 - t * t) * (1.0 + (3 * 0.044715) * g2))
    ua_ref[...] = g * half
    copy.wait()


def main_kernel(yh_ref, own_ref, rec_ref, w_ref, ga_ref, ua_ref, gg_ref, ug_ref, acc_ref, nat_ref):
    step = pl.program_id(0)

    @pl.when(step == 0)
    def _():
        acc_ref[...] = jnp.zeros_like(acc_ref)

    x_all = jnp.concatenate([parts(own_ref, step), parts(rec_ref, step)], axis=0)
    acc_ref[...] += jnp.dot(x_all, w_ref[...], preferred_element_type=jnp.float32)

    @pl.when(step == NSTEP - 1)
    def _():
        n = acc_ref.shape[1]
        yh = yh_ref[0]
        for j in range(0, n, LANES):
            w = min(LANES, n - j)
            for h in range(2):
                at = yh if h == 0 else 1 - yh
                for r in range(2):
                    row = (4 * h + r) * Z
                    part = acc_ref[row : row + Z, j : j + w] + acc_ref[row + 2 * Z : row + 3 * Z, j : j + w]
                    if w < LANES:
                        part = jnp.concatenate([part, jnp.zeros((Z, LANES - w), jnp.float32)], axis=1)
                    nat_ref[j // LANES, pl.ds(at * 2 + r, Z, stride=4), :] = part
            hidden = nat_ref[j // LANES].T[:w]
            gg_ref[j : j + w, :] = hidden * ga_ref[j : j + w, :]
            ug_ref[j : j + w, :] = hidden * ua_ref[j : j + w, :]


def whole(*shape):
    return pl.BlockSpec(shape, lambda i: (0,) * len(shape))


def run_factors(weight, gate, up, interpret=False):
    shape = jax.ShapeDtypeStruct(gate.shape, jnp.float32)
    vmem = pl.BlockSpec(memory_space=pltpu.VMEM)
    return pl.pallas_call(
        factor_kernel,
        in_specs=[pl.BlockSpec(memory_space=pl.ANY), vmem, vmem],
        out_specs=(pl.BlockSpec(memory_space=pl.ANY), vmem, vmem),
        out_shape=(jax.ShapeDtypeStruct(weight.shape, weight.dtype), shape, shape),
        scratch_shapes=[pltpu.SemaphoreType.DMA],
        cost_estimate=pl.CostEstimate(
            flops=20 * gate.size, transcendentals=gate.size, bytes_accessed=12 * gate.size + 4 * weight.size
        ),
        compiler_params=pltpu.CompilerParams(vmem_limit_bytes=STAGE_VMEM),
        name="factors",
        interpret=interpret,
    )(weight, gate, up)


def run_main(yh, own, rec, weight, ga, ua, interpret=False):
    n, rows = ga.shape
    shape = jax.ShapeDtypeStruct((n, rows), jnp.float32)
    return pl.pallas_call(
        main_kernel,
        grid=(NSTEP,),
        in_specs=[
            pl.BlockSpec(memory_space=pltpu.SMEM),
            whole(Z * ROWS, LANES),
            whole(Z * ROWS, LANES),
            pl.BlockSpec((KSTEP * LANES, n), lambda i: (i, 0)),
            whole(n, rows),
            whole(n, rows),
        ],
        out_specs=[whole(n, rows), whole(n, rows)],
        out_shape=(shape, shape),
        scratch_shapes=[
            pltpu.VMEM((2 * rows, n), jnp.float32),
            pltpu.VMEM(((n + LANES - 1) // LANES, rows, LANES), jnp.float32),
        ],
        compiler_params=pltpu.CompilerParams(vmem_limit_bytes=VMEM),
        name="main",
        interpret=interpret,
    )(yh, own, rec, weight, ga, ua)


def spread(v, axes):
    n = lax.axis_size(axes)
    return lax.all_to_all(jnp.broadcast_to(v[None], (n,) + v.shape), axes, 0, 0, tiled=True)


def steps(cotangent, mlp_out, post_gain, down_weight, gate_pre, up_pre):
    weight = lax.all_gather(down_weight.T, DP, axis=0, tiled=True)
    message = pl.pallas_call(
        pre_kernel,
        in_specs=[pl.BlockSpec(memory_space=pltpu.HBM)] * 3,
        out_shape=jax.ShapeDtypeStruct((ROWS + GROWS, LANES), jnp.float32),
        scratch_shapes=[
            pltpu.VMEM(cotangent.shape, cotangent.dtype),
            pltpu.VMEM(mlp_out.shape, mlp_out.dtype),
            pltpu.VMEM(post_gain.shape, post_gain.dtype),
            pltpu.SemaphoreType.DMA((3,)),
        ],
        compiler_params=pltpu.CompilerParams(vmem_limit_bytes=VMEM),
        name="pre",
    )(cotangent, mlp_out, post_gain)
    got = lax.all_gather(message.astype(jnp.float16), "z", axis=0)
    own = got[:, :ROWS].reshape(Z * ROWS, LANES)
    other = lax.ppermute(own, "yh", [(0, 1), (1, 0)])
    terms = got[:, ROWS:].astype(jnp.float32)
    expo = terms[:, 2 * KT : 2 * KT + 1]
    top = jnp.max(expo, axis=0)
    line = jnp.sum((terms[:, :KT] + terms[:, KT : 2 * KT] * (1.0 / LOW)) * jnp.exp2(expo - top), axis=0)
    line = jnp.concatenate([line, jnp.broadcast_to(top, (4, LANES))], axis=0).astype(jnp.float16)
    lines = spread(line, PLANE).astype(jnp.float32)
    gain_grad = jnp.sum(lines[:, :KT] * jnp.exp2(lines[:, KT : KT + 1]), axis=0).reshape(D)
    staged, ga, ua = run_factors(weight, gate_pre.T, up_pre.T)
    gate_grad, up_grad = run_main(
        lax.axis_index("yh").reshape(1), own.astype(jnp.float32), other.astype(jnp.float32), staged, ga, ua
    )
    return (gate_grad.T, up_grad.T, gain_grad)


def solution(mesh):
    finer = Mesh(mesh.devices.reshape(2, 4, 2, Z, 2), ALL)
    in_specs = (P(ALL, None), P(ALL, None), P(), P(MP, DP), P(DP, MP), P(DP, MP))
    out_specs = (P(DP, MP), P(DP, MP), P())
    return jax.shard_map(steps, mesh=finer, in_specs=in_specs, out_specs=out_specs, check_vma=False)
```

```python
import jax
import jax.numpy as jnp
from jax import lax
from jax.experimental import pallas as pl
from jax.experimental.pallas import tpu as pltpu
from jax.sharding import Mesh
from jax.sharding import PartitionSpec as P


D = 4608
DP = ("yl", "x", "c")
MP = ("z", "yh")
ALL = DP + MP
PLANE = ("c", "yh", "yl", "x")
epsilon = 1e-06

LANES = 128
KT = D // LANES
ROWS = 80
GROWS = 72
Z = 32
LOW = 256.0
VMEM = 20 << 20
PRE_VMEM = 20 << 20
STAGE_VMEM = 46 << 20


def pre_kernel(c_hbm, y_hbm, g_hbm, m_ref, c_ref, y_ref, g_ref, sems):
    pairs = ((c_hbm, c_ref), (y_hbm, y_ref), (g_hbm, g_ref))
    copies = [pltpu.make_async_copy(src, dst, sems.at[i]) for i, (src, dst) in enumerate(pairs)]
    for copy in copies:
        copy.start()
    for copy in copies:
        copy.wait()
    y = y_ref[...].astype(jnp.float32)
    c = c_ref[...].astype(jnp.float32)
    gain = jnp.broadcast_to(g_ref[...].reshape(1, D), (1, D))
    rm = jnp.sqrt(jnp.sum(y * y, axis=1, keepdims=True) / D + epsilon)
    gp = jnp.sum(c * (y / rm), axis=0, keepdims=True)
    scaled = c * gain
    ps = jnp.sum(scaled * y, axis=1, keepdims=True)
    og = scaled / rm - y * (ps / (D * (rm * rm * rm)))
    top = jnp.max(jnp.abs(og), axis=1, keepdims=True)
    e = jnp.clip(jnp.ceil(jnp.log2(jnp.maximum(top, 1e-37))), -100.0, 100.0)
    q = og * jnp.exp2(-e)
    gtop = jnp.max(jnp.abs(gp), axis=1, keepdims=True)
    ge = jnp.clip(jnp.ceil(jnp.log2(jnp.maximum(gtop, 1e-37))), -100.0, 100.0)
    gx = gp * jnp.exp2(-ge)
    hi = gx.astype(jnp.bfloat16).astype(jnp.float32)
    lo = (gx - hi) * LOW
    for k in range(KT):
        m_ref[2 * k : 2 * k + 2, :] = q[:, LANES * k : LANES * (k + 1)]
        m_ref[ROWS + k : ROWS + k + 1, :] = hi[:, LANES * k : LANES * (k + 1)]
        m_ref[ROWS + KT + k : ROWS + KT + k + 1, :] = lo[:, LANES * k : LANES * (k + 1)]
    m_ref[2 * KT : 2 * KT + 2, :] = jnp.broadcast_to(e, (2, LANES))
    m_ref[2 * KT + 2 : 2 * KT + 3, :] = jnp.broadcast_to(ge, (1, LANES))
    m_ref[2 * KT + 3 : ROWS, :] = jnp.zeros((ROWS - 2 * KT - 3, LANES), jnp.float32)


KSTEP = 12
NSTEP = KT // KSTEP


def parts(src_ref, step):
    scales = [jnp.exp2(src_ref[pl.ds(2 * KT + r, Z, stride=ROWS), :]) for r in range(2)]
    his, los = [], []
    for kk in range(KSTEP):
        x = jnp.concatenate(
            [src_ref[pl.ds(2 * (step * KSTEP + kk) + r, Z, stride=ROWS), :] * scales[r] for r in range(2)], axis=0
        )
        hi = x.astype(jnp.bfloat16)
        his.append(hi)
        los.append((x - hi.astype(jnp.float32)).astype(jnp.bfloat16))
    return jnp.concatenate([jnp.concatenate(his, axis=1), jnp.concatenate(los, axis=1)], axis=0)


def factor_kernel(w_hbm, gate_ref, up_ref, w_out, ga_ref, ua_ref, sem):
    copy = pltpu.make_async_copy(w_hbm, w_out, sem)
    copy.start()
    g = gate_ref[...].astype(jnp.float32)
    u = up_ref[...].astype(jnp.float32)
    k0 = 0.7978845608028654
    g2 = g * g
    t = jnp.tanh(k0 * (g + 0.044715 * (g2 * g)))
    half = 0.5 * (1.0 + t)
    ga_ref[...] = u * (half + (0.5 * k0) * g * (1.0 - t * t) * (1.0 + (3 * 0.044715) * g2))
    ua_ref[...] = g * half
    copy.wait()


def main_kernel(yh_ref, own_ref, rec_ref, w_ref, ga_ref, ua_ref, gg_ref, ug_ref, acc_ref, nat_ref):
    total = None
    for step in range(NSTEP):
        x_all = jnp.concatenate([parts(own_ref, step), parts(rec_ref, step)], axis=0)
        weight = w_ref[step * KSTEP * LANES : (step + 1) * KSTEP * LANES, :]
        part = jnp.dot(x_all, weight, preferred_element_type=jnp.float32)
        total = part if total is None else total + part
    acc_ref[...] = total

    n = acc_ref.shape[1]
    yh = yh_ref[0]
    for j in range(0, n, LANES):
        w = min(LANES, n - j)
        for h in range(2):
            at = yh if h == 0 else 1 - yh
            for r in range(2):
                row = (4 * h + r) * Z
                part = acc_ref[row : row + Z, j : j + w] + acc_ref[row + 2 * Z : row + 3 * Z, j : j + w]
                if w < LANES:
                    part = jnp.concatenate([part, jnp.zeros((Z, LANES - w), jnp.float32)], axis=1)
                nat_ref[j // LANES, pl.ds(at * 2 + r, Z, stride=4), :] = part
        hidden = nat_ref[j // LANES].T[:w]
        gg_ref[j : j + w, :] = hidden * ga_ref[j : j + w, :]
        ug_ref[j : j + w, :] = hidden * ua_ref[j : j + w, :]


def run_factors(weight, gate, up, interpret=False):
    shape = jax.ShapeDtypeStruct(gate.shape, jnp.float32)
    vmem = pl.BlockSpec(memory_space=pltpu.VMEM)
    return pl.pallas_call(
        factor_kernel,
        in_specs=[pl.BlockSpec(memory_space=pl.ANY), vmem, vmem],
        out_specs=(pl.BlockSpec(memory_space=pl.ANY), vmem, vmem),
        out_shape=(jax.ShapeDtypeStruct(weight.shape, weight.dtype), shape, shape),
        scratch_shapes=[pltpu.SemaphoreType.DMA],
        cost_estimate=pl.CostEstimate(
            flops=20 * gate.size, transcendentals=gate.size, bytes_accessed=12 * gate.size + 4 * weight.size
        ),
        compiler_params=pltpu.CompilerParams(vmem_limit_bytes=STAGE_VMEM),
        name="factors",
        interpret=interpret,
    )(weight, gate, up)


def run_main(yh, own, rec, weight, ga, ua, interpret=False):
    n, rows = ga.shape
    shape = jax.ShapeDtypeStruct((n, rows), jnp.float32)
    return pl.pallas_call(
        main_kernel,
        in_specs=[pl.BlockSpec(memory_space=pltpu.SMEM)] + [pl.BlockSpec(memory_space=pltpu.VMEM)] * 5,
        out_specs=[pl.BlockSpec(memory_space=pltpu.VMEM)] * 2,
        out_shape=(shape, shape),
        scratch_shapes=[
            pltpu.VMEM((2 * rows, n), jnp.float32),
            pltpu.VMEM(((n + LANES - 1) // LANES, rows, LANES), jnp.float32),
        ],
        compiler_params=pltpu.CompilerParams(vmem_limit_bytes=VMEM),
        name="main",
        interpret=interpret,
    )(yh, own, rec, weight, ga, ua)


def spread(v, axes):
    n = lax.axis_size(axes)
    return lax.all_to_all(jnp.broadcast_to(v[None], (n,) + v.shape), axes, 0, 0, tiled=True)


def steps(cotangent, mlp_out, post_gain, down_weight, gate_pre, up_pre):
    weight = lax.all_gather(down_weight.T, DP, axis=0, tiled=True)
    message = pl.pallas_call(
        pre_kernel,
        in_specs=[pl.BlockSpec(memory_space=pltpu.HBM)] * 3,
        out_shape=jax.ShapeDtypeStruct((ROWS + GROWS, LANES), jnp.float32),
        scratch_shapes=[
            pltpu.VMEM(cotangent.shape, cotangent.dtype),
            pltpu.VMEM(mlp_out.shape, mlp_out.dtype),
            pltpu.VMEM(post_gain.shape, post_gain.dtype),
            pltpu.SemaphoreType.DMA((3,)),
        ],
        compiler_params=pltpu.CompilerParams(vmem_limit_bytes=PRE_VMEM),
        name="pre",
    )(cotangent, mlp_out, post_gain)
    got = lax.all_gather(message.astype(jnp.float16), "z", axis=0)
    own = got[:, :ROWS].reshape(Z * ROWS, LANES)
    other = lax.ppermute(own, "yh", [(0, 1), (1, 0)])
    terms = got[:, ROWS:].astype(jnp.float32)
    expo = got[:, 2 * KT + 2 : 2 * KT + 3].astype(jnp.float32)
    top = jnp.max(expo, axis=0)
    line = jnp.sum((terms[:, :KT] + terms[:, KT : 2 * KT] * (1.0 / LOW)) * jnp.exp2(expo - top), axis=0)
    line = jnp.concatenate([line, jnp.broadcast_to(top, (4, LANES))], axis=0).astype(jnp.float16)
    lines = spread(line, PLANE).astype(jnp.float32)
    gain_grad = jnp.sum(lines[:, :KT] * jnp.exp2(lines[:, KT : KT + 1]), axis=0).reshape(D)
    staged, ga, ua = run_factors(weight, gate_pre.T, up_pre.T)
    gate_grad, up_grad = run_main(
        lax.axis_index("yh").reshape(1), own.astype(jnp.float32), other.astype(jnp.float32), staged, ga, ua
    )
    return (gate_grad.T, up_grad.T, gain_grad)


def solution(mesh):
    finer = Mesh(mesh.devices.reshape(2, 4, 2, Z, 2), ALL)
    in_specs = (P(ALL, None), P(ALL, None), P(), P(MP, DP), P(DP, MP), P(DP, MP))
    out_specs = (P(DP, MP), P(DP, MP), P())
    return jax.shard_map(steps, mesh=finer, in_specs=in_specs, out_specs=out_specs, check_vma=False)
```
